32 devices in a mesh: expert: 4 (over x, core), rows: 8 (over z, y).
Axes of the slice: x: 2, y: 2, z: 4, core: 2. Of those that a mesh axis runs over, the one named last changes fastest.
Arguments:
- step: int32 [], replicated, may hold values from 2 to 8
- gradient: bfloat16 [4, 4096, 14336], P('expert', 'rows'), may hold values from -8 to 8
- weight: bfloat16 [4, 4096, 14336], P('expert', 'rows'), may hold values from -0.119628906 to 0.119628906
- row_state: float32 [4, 4096], P('expert', 'rows'), may hold values from 0.3 to 3
- col_state: float32 [4, 14336], P('expert', 'rows'), may hold values from 0.3 to 3
- prev_msq: float32 [4, 8], P('expert', 'rows'), may hold values from 2 to 500
Outputs:
- new_weight: bfloat16 [4, 4096, 14336], P('expert', 'rows')
- new_row_state: float32 [4, 4096], P('expert', 'rows')
- new_col_state: float32 [4, 14336], P('expert', 'rows')
- new_msq: float32 [4, 8], P('expert', 'rows')
The draws below stay inside these ranges and needn't reach their ends.
All inputs are finite; a program needn't handle non-finite values.
Results may differ from the reference program's by a relative error of at most 0.001.
Values sent between devices are 32-bit elements; how exact they have to be, the bound alone decides.
A program may use at most 128 MiB of HBM per device.

```python
import math
import jax
import jax.numpy as jnp
from jax import lax

D = 4096
FF = 14336
EXPERTS = 4
N_ROWS = 8


def draw_gradient(key, part):
    row_blocks = 2 * N_ROWS
    block_rows = D // row_blocks
    col_blocks = FF // 8
    level_key = jax.random.fold_in(key, 11)
    noise_key = jax.random.fold_in(key, 23)
    spread = 1.0
    noise = jax.random.normal(noise_key, (EXPERTS, row_blocks, block_rows, col_blocks, 8), jnp.float32)
    levels = jnp.exp(jax.random.uniform(level_key, (EXPERTS, row_blocks, 1, col_blocks, 1), jnp.float32, -spread, spread))
    values = jnp.clip(noise * levels, -8.0, 8.0)
    return values.reshape(EXPERTS, D, FF).astype(jnp.bfloat16)


def block_scale(rng, extent, pieces, smallest, high):
    factor_of, own = 1.0, jax.random.fold_in(rng, 6)
    for dim, parts in pieces:
        draws = jnp.exp(jax.random.uniform(jax.random.fold_in(own, dim), (parts,), jnp.float32, smallest / len(pieces), high / len(pieces)))
        factor_of = factor_of * jnp.repeat(draws, extent[dim] // parts).reshape([-1 if axis == dim else 1 for axis in range(len(extent))])
    return factor_of


def bell_draw(stream_key, dims, width, reach, shards=(), dtype=jnp.bfloat16):
    result = jax.random.normal(stream_key, dims, jnp.float32) * width
    if len(shards) > 0:
        result = block_scale(stream_key, dims, shards, -0.22, 0.18) * result
    return jnp.clip(result, min=-reach, max=reach).astype(dtype)


def setup_inputs(seed: int = 0) -> dict:
    key_of = jax.random.split(jax.random.key(seed), 7)
    step = jax.random.randint(key_of[0], (), 2, 9).astype(jnp.int32)
    gradient = draw_gradient(jax.random.fold_in(key_of[6], 71), 0)
    weight = bell_draw(key_of[2], (EXPERTS, D, FF), 0.02, 0.119628906, ((0, 4), (1, 8)))
    row_state = jnp.clip(jnp.exp(math.log(3.0) - 2.3025851 * jax.random.uniform(key_of[3], (EXPERTS, D), jnp.float32) ** block_scale(key_of[3], (EXPERTS, D), ((0, 4), (1, 8)), -0.2, 0.2)), 0.3, 3.0)
    col_state = jnp.clip(jnp.exp(math.log(3.0) - 2.3025851 * jax.random.uniform(key_of[4], (EXPERTS, FF), jnp.float32) ** block_scale(key_of[4], (EXPERTS, FF), ((0, 4), (1, 8)), -0.2, 0.2)), 0.3, 3.0)
    prev_msq = jnp.clip(jnp.exp(math.log(500.0) - 5.521461 * jax.random.uniform(key_of[5], (EXPERTS, N_ROWS), jnp.float32) ** block_scale(key_of[5], (EXPERTS, N_ROWS), ((0, 4), (1, 8)), -0.2, 0.2)), 2.0, 500.0)
    return dict(step=step, gradient=gradient, weight=weight, row_state=row_state, col_state=col_state, prev_msq=prev_msq)


def one_expert(inputs):
    gradient, weight, row_state, col_state, beta, clip = inputs
    grad = gradient.astype(jnp.float32)
    squares = grad * grad + 1e-30
    new_row = beta * row_state + (1.0 - beta) * lax.optimization_barrier(jnp.mean(squares, axis=1))
    new_col = beta * col_state + (1.0 - beta) * lax.optimization_barrier(jnp.sum(squares, axis=0)) / D
    row_mean = jnp.mean(new_row)
    scaled = new_row[:, None] * new_col[None, :] / row_mean
    update = grad / jnp.sqrt(scaled) / clip
    new_weight = (weight.astype(jnp.float32) - 0.01 * update).astype(jnp.bfloat16)
    blocks = (update * update).reshape(N_ROWS, D // N_ROWS, FF)
    new_msq = lax.optimization_barrier(jnp.mean(blocks, axis=(1, 2)))
    return (new_weight, new_row, new_col, new_msq)

def reference(step, gradient, weight, row_state, col_state, prev_msq):
    beta = 1.0 - step.astype(jnp.float32) ** (-0.8)
    clip = jnp.sqrt(jnp.mean(prev_msq))
    count = gradient.shape[0]
    betas = jnp.full((count,), beta, jnp.float32)
    clips = jnp.full((count,), clip, jnp.float32)
    new_weight, new_row, new_col, new_msq = lax.map(one_expert, (gradient, weight, row_state, col_state, betas, clips))
    return (new_weight, new_row, new_col, new_msq)
```

```python
import functools

import jax
import jax.numpy as jnp
from jax import lax
from jax.experimental import pallas as pl
from jax.experimental.pallas import tpu as pltpu
from jax.sharding import PartitionSpec as P

MESH = pl.DeviceIdType.MESH
RATE = 0.01
TINY = 1e-30
LANES = 128
ROWS = 16
UNROLL = 4
SLOTS = 4


def lane_sum(x):
    total = x[:, :LANES]
    for k in range(1, x.shape[1] // LANES):
        total = total + x[:, k * LANES : (k + 1) * LANES]
    return total


def statistics_kernel(
    n, experts, early, step_ref, prev_ref, row_hbm, col_hbm, g_hbm, w_hbm,
    u_out, w_out, factor_out, new_row_out, new_col_out, msq_out,
    acc, scale_ref, energy, part, parts_in, message, messages_in, clip_out, clips_in,
    row_ref, col_ref, small_sem, g_sem, w_sem,
    clip_send, clip_recv, part_send, part_recv, gather_send, gather_recv,
):
    me = lax.axis_index("rows")
    mine = lax.axis_index("expert")
    rows, columns = u_out.shape
    width = columns // n

    def column_slice(c):
        return pl.ds(pl.multiple_of(c * width, LANES), width)

    def partner(k):
        peer, bit = 0, 1
        while bit < n:
            peer = peer + bit * ((me // bit + k // bit) % 2)
            bit *= 2
        return peer

    def chunk_of(s):
        return partner(n - 1 - s)

    def g_copy(s):
        cols = column_slice(chunk_of(s))
        return pltpu.make_async_copy(g_hbm.at[:, cols], w_out.at[:, cols], g_sem.at[s])

    def w_copy(s):
        cols = column_slice(s)
        return pltpu.make_async_copy(w_hbm.at[:, cols], w_out.at[:, cols], w_sem.at[s])

    def clip_copy(k):
        peer = lax.rem(mine + k, experts)
        return pltpu.make_async_remote_copy(
            src_ref=clip_out, dst_ref=clips_in.at[k - 1], send_sem=clip_send.at[k - 1],
            recv_sem=clip_recv.at[k - 1], device_id={"expert": peer}, device_id_type=MESH,
        )

    def part_copy(s):
        c = chunk_of(s)
        return pltpu.make_async_remote_copy(
            src_ref=part.at[s], dst_ref=parts_in.at[s], send_sem=part_send.at[s],
            recv_sem=part_recv.at[s], device_id={"rows": c}, device_id_type=MESH,
        )

    def gather_copy(k):
        peer = partner(k)
        return pltpu.make_async_remote_copy(
            src_ref=message, dst_ref=messages_in.at[k - 1], send_sem=gather_send.at[k - 1],
            recv_sem=gather_recv.at[k - 1], device_id={"rows": peer}, device_id_type=MESH,
        )

    pairs = ((row_hbm, row_ref), (col_hbm, col_ref))
    small = [pltpu.make_async_copy(src, dst, small_sem.at[k]) for k, (src, dst) in enumerate(pairs)]
    for copy in small:
        copy.start()
    for s in range(n):
        g_copy(s).start()

    barrier = pltpu.get_barrier_semaphore()
    for k in range(1, n):
        pl.semaphore_signal(barrier, inc=1, device_id={"rows": lax.rem(me + k, n)}, device_id_type=MESH)
    for k in range(1, experts):
        pl.semaphore_signal(barrier, inc=1, device_id={"expert": lax.rem(mine + k, experts)}, device_id_type=MESH)

    acc[...] = jnp.zeros_like(acc)
    for copy in small:
        copy.wait()
    clip_out[...] = jnp.full((1, LANES), prev_ref[0], jnp.float32)
    beta = 1.0 - jnp.exp(-0.8 * jnp.log(jnp.full((1, LANES), step_ref[0], jnp.int32).astype(jnp.float32)))

    def chunk(s):
        cols = column_slice(chunk_of(s))
        g_copy(s).wait()

        def body(i, carry):
            at = pl.ds(pl.multiple_of(i * ROWS, ROWS), ROWS)
            x = w_out[at, cols].astype(jnp.float32)
            u_out[at, cols] = x
            squares = x * x
            acc[at, :] += lane_sum(squares)
            return carry + (squares[: ROWS // 2] + squares[ROWS // 2 :])

        col = lax.fori_loop(0, rows // ROWS, body, jnp.zeros((ROWS // 2, width), jnp.float32), unroll=UNROLL)
        part[s] = jnp.sum(col, axis=0, keepdims=True)

    def scaled(s):
        cols = column_slice(s)

        def body(i, carry):
            at = pl.ds(pl.multiple_of(i * ROWS, ROWS), ROWS)
            scale = jnp.concatenate([scale_ref[at, :]] * (width // LANES), axis=1)
            u = u_out[at, cols] * scale
            u_out[at, cols] = u
            squares = u * u
            return carry + (squares[: ROWS // 2] + squares[ROWS // 2 :])

        col = lax.fori_loop(0, rows // ROWS, body, jnp.zeros((ROWS // 2, width), jnp.float32), unroll=2)
        energy[:, cols] = jnp.sum(col, axis=0, keepdims=True)

    half = n // 2

    @pl.loop(0, half)
    def _(s):
        chunk(s)

    pl.semaphore_wait(barrier, n - 1 + experts - 1)
    for k in range(1, experts):
        clip_copy(k).start()
    for s in range(half):
        part_copy(s).start()

    @pl.loop(half, n - 1)
    def _(s):
        chunk(s)
        part_copy(s).start()

    chunk(n - 1)
    for s in range(n):
        w_copy(s).start()

    beta_rows = jnp.concatenate([beta] * (rows // LANES), axis=1)
    sums = jnp.sum(jnp.transpose(acc[...]), axis=0, keepdims=True)
    new_row = beta_rows * row_ref[...] + (1.0 - beta_rows) * (sums * (1.0 / columns) + TINY)
    new_row_out[...] = new_row
    scale_ref[...] = jnp.transpose(jnp.broadcast_to(lax.rsqrt(new_row), (LANES, rows)))
    share = lane_sum(new_row)

    @pl.loop(0, early)
    def _(s):
        scaled(s)

    clips = clip_out[...]
    for k in range(1, experts):
        clip_copy(k).wait()
        clips = clips + clips_in[k - 1]
    total = part[n - 1]
    for s in range(n - 1):
        part_copy(s).wait()
        total = total + parts_in[s]
    beta_cols = jnp.concatenate([beta] * (width // LANES), axis=1)
    new_col = beta_cols * col_ref[...] + (1.0 - beta_cols) * (total * (1.0 / (rows * n)) + TINY)
    message[:, :width] = new_col
    message[:, width : width + LANES] = share
    message[:, width + LANES :] = clips
    for k in reversed(range(1, n)):
        gather_copy(k).start()
    new_col_out[...] = new_col

    @pl.loop(early, n)
    def _(s):
        scaled(s)

    for s in range(n):
        w_copy(s).wait()

    for k in reversed(range(1, n)):
        gather_copy(k).wait()
        share = share + messages_in[k - 1, :, width : width + LANES]
        clips = clips + messages_in[k - 1, :, width + LANES :]
    row_mean = jnp.sum(share, axis=1, keepdims=True) * (1.0 / (rows * n))
    clip_square = clips[:, :1] * (1.0 / (n * experts))
    common = RATE * jnp.sqrt(row_mean) * lax.rsqrt(clip_square)
    moved = jnp.zeros((1, LANES), jnp.float32)
    for k in range(n):
        cols = column_slice(partner(k))
        column = new_col if k == 0 else messages_in[k - 1, :, :width]
        factor = lax.rsqrt(column) * common
        factor_out[:, cols] = factor
        moved = moved + lane_sum(energy[:, cols] * (factor * factor))
    msq_out[...] = moved * (1.0 / (RATE * RATE * rows * columns))


def update_kernel(
    block, u_ref, w_ref, factor_ref, row_ref, col_ref, msq_ref,
    new_w_hbm, new_row_out, new_col_out, msq_out, stage, sem,
):
    rows, columns = u_ref.shape
    blocks = columns // block

    def out_copy(b):
        slot = lax.rem(b, SLOTS)
        cols = pl.ds(pl.multiple_of(b * block, LANES), block)
        return pltpu.make_async_copy(stage.at[slot], new_w_hbm.at[:, cols], sem.at[slot])

    @pl.loop(0, blocks)
    def _(b):
        cols = pl.ds(pl.multiple_of(b * block, LANES), block)
        slot = lax.rem(b, SLOTS)

        @pl.when(b >= SLOTS)
        def _():
            out_copy(b - SLOTS).wait()

        factor = jnp.broadcast_to(factor_ref[:, cols], (ROWS, block))

        @pl.loop(0, rows // ROWS, unroll=UNROLL)
        def _(i):
            at = pl.ds(pl.multiple_of(i * ROWS, ROWS), ROWS)
            new = w_ref[at, cols].astype(jnp.float32) - u_ref[at, cols] * factor
            stage[slot, at, :] = new.astype(jnp.bfloat16)

        out_copy(b).start()

    new_row_out[...] = row_ref[...]
    new_col_out[...] = col_ref[...]
    msq_out[...] = jnp.sum(msq_ref[...], axis=1, keepdims=True)
    for b in range(max(blocks - SLOTS, 0), blocks):
        out_copy(b).wait()


def block_width(columns):
    tiles = columns // LANES
    for d in (8, 7, 4, 2, 1):
        if tiles % d == 0:
            return d * LANES


def shards(step, gradient, weight, row_state, col_state, prev_msq):
    _, rows, columns = gradient.shape
    n = lax.axis_size("rows")
    experts = lax.axis_size("expert")
    width = columns // n
    f32, bf16 = jnp.float32, gradient.dtype
    vmem = pl.BlockSpec(memory_space=pltpu.VMEM)
    hbm = pl.BlockSpec(memory_space=pltpu.HBM)
    dma = pltpu.SemaphoreType.DMA
    u, w, factor, new_row, new_col, msq = pl.pallas_call(
        functools.partial(statistics_kernel, n, experts, n // 4),
        out_shape=[
            pltpu.VMEM((rows, columns), f32),
            pltpu.VMEM((rows, columns), bf16),
            pltpu.VMEM((1, columns), f32),
            pltpu.VMEM((1, rows), f32),
            pltpu.VMEM((1, width), f32),
            pltpu.VMEM((1, LANES), f32),
        ],
        in_specs=[pl.BlockSpec(memory_space=pltpu.SMEM)] * 2 + [hbm] * 4,
        out_specs=[vmem] * 6,
        scratch_shapes=[
            pltpu.VMEM((rows, LANES), f32),
            pltpu.VMEM((rows, LANES), f32),
            pltpu.VMEM((1, columns), f32),
            pltpu.VMEM((n, 1, width), f32),
            pltpu.VMEM((n - 1, 1, width), f32),
            pltpu.VMEM((1, width + 2 * LANES), f32),
            pltpu.VMEM((n - 1, 1, width + 2 * LANES), f32),
            pltpu.VMEM((1, LANES), f32),
            pltpu.VMEM((experts - 1, 1, LANES), f32),
            pltpu.VMEM((1, rows), f32),
            pltpu.VMEM((1, width), f32),
            dma((2,)), dma((n,)), dma((n,)), dma((experts - 1,)), dma((experts - 1,)),
            dma((n - 1,)), dma((n - 1,)), dma((n - 1,)), dma((n - 1,)),
        ],
        compiler_params=pltpu.CompilerParams(
            collective_id=0, has_side_effects=True, vmem_limit_bytes=8 * 2**20
        ),
        name="statistics",
    )(
        step.reshape(1), prev_msq.reshape(1),
        *(
            pltpu.with_memory_space_constraint(x, pltpu.HBM)
            for x in (
                row_state, col_state,
                gradient.reshape(rows, columns), weight.reshape(rows, columns),
            )
        ),
    )
    block = block_width(columns)
    new_weight, new_row, new_col, msq = pl.pallas_call(
        functools.partial(update_kernel, block),
        out_shape=[
            jax.ShapeDtypeStruct((rows, columns), bf16),
            jax.ShapeDtypeStruct((1, rows), f32),
            jax.ShapeDtypeStruct((1, width), f32),
            jax.ShapeDtypeStruct((1, 1), f32),
        ],
        in_specs=[vmem] * 6,
        out_specs=[hbm, vmem, vmem, vmem],
        scratch_shapes=[pltpu.VMEM((SLOTS, rows, block), bf16), dma((SLOTS,))],
        compiler_params=pltpu.CompilerParams(vmem_limit_bytes=8 * 2**20),
        name="update",
    )(u, w, factor, new_row, new_col, msq)
    return (new_weight.reshape(1, rows, columns), new_row, new_col, msq)


def solution(mesh):
    split = P("expert", "rows")
    whole = P("expert", "rows", None)
    return jax.shard_map(
        shards,
        mesh=mesh,
        in_specs=(P(), whole, whole, split, split, split),
        out_specs=(whole, split, split, split),
        check_vma=False,
    )
```

```python
import functools

import jax
import jax.numpy as jnp
from jax import lax
from jax.experimental import pallas as pl
from jax.experimental.pallas import tpu as pltpu
from jax.sharding import PartitionSpec as P

MESH = pl.DeviceIdType.MESH
RATE = 0.01
TINY = 1e-30
LANES = 128
ROWS = 16
BLOCK = 128
DEPTH = 4
EARLY = 2
SLOTS = 4
ROW = [slice(r, r + ROWS) for r in range(0, BLOCK, ROWS)]
TILE = [slice(k * LANES, (k + 1) * LANES) for k in range(16)]


def lane_sum(x):
    total = x[:, :LANES]
    for k in range(1, x.shape[1] // LANES):
        total = total + x[:, k * LANES : (k + 1) * LANES]
    return total


def statistics_kernel(
    n, experts, step_ref, prev_ref, row_hbm, col_hbm, g_hbm, w_hbm,
    u_out, w_out, factor_out, common_out, new_row_out, new_col_out, moved_out,
    acc, scale_ref, energy, part, parts_in, message, messages_in, clip_out, clips_in,
    row_ref, col_ref, small_sem, g_sem, w_sem,
    clip_send, clip_recv, part_send, part_recv, gather_send, gather_recv,
):
    me = lax.axis_index("rows")
    mine = lax.axis_index("expert")
    rows, columns = u_out.shape
    width = columns // n

    def column_slice(c):
        return pl.ds(pl.multiple_of(c * width, LANES), width)

    tiles = tile_count(width)

    def strip_slice(c, first):
        return pl.ds(pl.multiple_of(c * width + first * LANES, LANES), tiles * LANES)

    def partner(k):
        peer, bit = 0, 1
        while bit < n:
            peer = peer + bit * ((me // bit + k // bit) % 2)
            bit *= 2
        return peer

    def chunk_of(s):
        return partner(n - 1 - s)

    def g_copy(s):
        cols = column_slice(chunk_of(s))
        return pltpu.make_async_copy(g_hbm.at[:, cols], w_out.at[:, cols], g_sem.at[lax.rem(s, DEPTH)])

    def w_copy(s):
        cols = column_slice(s)
        return pltpu.make_async_copy(w_hbm.at[:, cols], w_out.at[:, cols], w_sem)

    def clip_copy(k):
        peer = lax.rem(mine + k, experts)
        return pltpu.make_async_remote_copy(
            src_ref=clip_out, dst_ref=clips_in.at[k - 1], send_sem=clip_send,
            recv_sem=clip_recv, device_id={"expert": peer}, device_id_type=MESH,
        )

    def part_copy(s):
        c = chunk_of(s)
        return pltpu.make_async_remote_copy(
            src_ref=part.at[s], dst_ref=parts_in.at[s], send_sem=part_send,
            recv_sem=part_recv, device_id={"rows": c}, device_id_type=MESH,
        )

    def gather_copy(k):
        peer = partner(k)
        return pltpu.make_async_remote_copy(
            src_ref=message, dst_ref=messages_in.at[k - 1], send_sem=gather_send,
            recv_sem=gather_recv.at[k - 1], device_id={"rows": peer}, device_id_type=MESH,
        )

    pairs = ((row_hbm, row_ref), (col_hbm, col_ref))
    small = [pltpu.make_async_copy(src, dst, small_sem.at[k]) for k, (src, dst) in enumerate(pairs)]
    for copy in small:
        copy.start()
    for s in range(DEPTH):
        g_copy(s).start()

    barrier = pltpu.get_barrier_semaphore()
    for k in range(1, n):
        pl.semaphore_signal(barrier, inc=1, device_id={"rows": lax.rem(me + k, n)}, device_id_type=MESH)
    for k in range(1, experts):
        pl.semaphore_signal(barrier, inc=1, device_id={"expert": lax.rem(mine + k, experts)}, device_id_type=MESH)

    clip_out[...] = jnp.full((1, LANES), prev_ref[0], jnp.float32)
    beta = 1.0 - jnp.exp(-0.8 * jnp.log(jnp.full((1, LANES), step_ref[0], jnp.int32).astype(jnp.float32)))

    def chunk(s):
        for first in range(0, width // LANES, tiles):
            strip = strip_slice(chunk_of(s), first)

            def body(i, carry):
                at = pl.ds(pl.multiple_of(i * BLOCK, BLOCK), BLOCK)
                source, target = w_out.at[at, strip], u_out.at[at, strip]
                carry = list(carry)
                for row in ROW:
                    for k in range(tiles):
                        x = source[row, TILE[k]].astype(jnp.float32)
                        target[row, TILE[k]] = x
                        squares = x * x
                        carry[k] = carry[k] + (squares[: ROWS // 2] + squares[ROWS // 2 :])
                return tuple(carry)

            zeros = (jnp.zeros((ROWS // 2, LANES), jnp.float32),) * tiles
            col = lax.fori_loop(0, rows // BLOCK, body, zeros)
            for k in range(tiles):
                part[s, :, (first + k) * LANES : (first + k + 1) * LANES] = jnp.sum(col[k], axis=0, keepdims=True)

    def scaled(s):
        for first in range(0, width // LANES, tiles):
            strip = strip_slice(s, first)

            def body(i, carry):
                at = pl.ds(pl.multiple_of(i * BLOCK, BLOCK), BLOCK)
                target, scales = u_out.at[at, strip], scale_ref.at[at]
                carry = list(carry)
                for row in ROW:
                    scale = scales[row, :]
                    for k in range(tiles):
                        u = target[row, TILE[k]] * scale
                        target[row, TILE[k]] = u
                        squares = u * u
                        carry[k] = carry[k] + (squares[: ROWS // 2] + squares[ROWS // 2 :])
                return tuple(carry)

            zeros = (jnp.zeros((ROWS // 2, LANES), jnp.float32),) * tiles
            col = lax.fori_loop(0, rows // BLOCK, body, zeros)
            for k in range(tiles):
                energy.at[:, strip][:, TILE[k]] = jnp.sum(col[k], axis=0, keepdims=True)

    half = n // 2

    @pl.loop(0, half)
    def _(s):
        g_copy(s).wait()
        g_copy(s + DEPTH).start()
        chunk(s)

    pl.semaphore_wait(barrier, n - 1 + experts - 1)
    for k in range(1, experts):
        clip_copy(k).start()
    for s in range(half):
        part_copy(s).start()

    @pl.loop(half, n - 1)
    def _(s):
        g_copy(s).wait()

        @pl.when(s + DEPTH < n)
        def _():
            g_copy(s + DEPTH).start()

        @pl.when(s + DEPTH >= n)
        def _():
            w_copy(chunk_of(s + DEPTH - n)).start()

        chunk(s)
        part_copy(s).start()

    g_copy(n - 1).wait()
    for s in range(DEPTH - 1, n - 1):
        w_copy(chunk_of(s)).start()
    chunk(n - 1)
    w_copy(chunk_of(n - 1)).start()

    for copy in small:
        copy.wait()
    beta_rows = jnp.concatenate([beta] * (rows // LANES), axis=1)
    squares = part[0]
    for s in range(1, n):
        squares = squares + part[s]
    share = lane_sum(row_ref[...]) * beta
    share = share + (1.0 - beta) * (lane_sum(squares) * (1.0 / columns) + TINY * (rows / LANES))
    share = jnp.broadcast_to(jnp.sum(share, axis=1, keepdims=True), (1, LANES))

    def whole_copy(ref, send, recv):
        return pltpu.make_async_remote_copy(
            src_ref=ref, dst_ref=ref, send_sem=send, recv_sem=recv,
            device_id={"rows": partner(1)}, device_id_type=MESH,
        )

    def respond():
        clips = clip_out[...]
        whole_copy(clips_in, clip_send, clip_recv).wait()
        for k in range(1, experts):
            clips = clips + clips_in[k - 1]
        whole_copy(parts_in, part_send, part_recv).wait_recv()
        total = part[n - 1]
        for s in range(n - 1):
            total = total + parts_in[s]
        beta_cols = jnp.concatenate([beta] * (width // LANES), axis=1)
        message[:, :width] = beta_cols * col_ref[...] + (1.0 - beta_cols) * (total * (1.0 / (rows * n)) + TINY)
        message[:, width : width + LANES] = share
        message[:, width + LANES :] = clips
        for k in reversed(range(1, n)):
            gather_copy(k).start()

    def row_sums(i):
        at = pl.ds(pl.multiple_of(i * ROWS, ROWS), ROWS)
        source = u_out.at[at]
        sums = [None] * 4
        for k in range(columns // LANES):
            x = source[:, k * LANES : (k + 1) * LANES]
            sums[k % 4] = x * x if k < 4 else sums[k % 4] + x * x
        acc[at, :] = (sums[0] + sums[1]) + (sums[2] + sums[3])

    middle = rows // ROWS // 2

    @pl.loop(0, middle)
    def _(i):
        row_sums(i)

    @pl.when(me != 0)
    def _():
        respond()

    @pl.loop(middle, rows // ROWS)
    def _(i):
        row_sums(i)

    sums = jnp.sum(jnp.transpose(acc[...]), axis=0, keepdims=True)
    new_row = beta_rows * row_ref[...] + (1.0 - beta_rows) * (sums * (1.0 / columns) + TINY)
    new_row_out[...] = new_row
    scale_ref[...] = jnp.transpose(jnp.broadcast_to(lax.rsqrt(new_row), (LANES, rows)))
    early = jnp.where(me == 0, n * EARLY // 8, 0)

    @pl.loop(0, early)
    def _(s):
        scaled(s)

    @pl.when(me == 0)
    def _():
        respond()

    @pl.loop(early, n)
    def _(s):
        scaled(s)

    pltpu.make_async_copy(w_hbm, w_out, w_sem).wait()

    new_col_out[...] = message[:, :width]
    whole_copy(parts_in, part_send, part_recv).wait_send()
    share, clips, moved = 0.0, 0.0, 0.0
    for k in range(n):
        cols = column_slice(partner(k))
        if k > 0:
            gather_copy(k).wait_recv()
        got = message[...] if k == 0 else messages_in[k - 1]
        inverse = lax.rsqrt(got[:, :width])
        factor_out[:, cols] = inverse
        share = share + got[:, width : width + LANES]
        clips = clips + got[:, width + LANES :]
        moved = moved + lane_sum(energy[:, cols] * (inverse * inverse))
    whole_copy(messages_in, gather_send, gather_recv.at[0]).wait_send()
    common_out[...] = RATE * jnp.sqrt(share * (1.0 / (rows * n))) * lax.rsqrt(clips * (1.0 / (n * experts)))
    moved_out[...] = moved


def update_kernel(
    block, u_ref, w_ref, factor_ref, common_ref, row_ref, col_ref, moved_ref,
    new_w_hbm, new_row_hbm, new_col_hbm, msq_hbm, stage, msq_ref, sem, small_sem,
):
    rows, columns = u_ref.shape
    blocks = columns // block
    common = common_ref[...]
    msq = moved_ref[...] * (common * common) * (1.0 / (RATE * RATE * rows * columns))
    msq_ref[...] = jnp.sum(msq, axis=1, keepdims=True)

    def out_copy(b):
        slot = lax.rem(b, SLOTS)
        cols = pl.ds(pl.multiple_of(b * block, LANES), block)
        return pltpu.make_async_copy(stage.at[slot], new_w_hbm.at[:, cols], sem.at[slot])

    pairs = ((row_ref, new_row_hbm), (col_ref, new_col_hbm), (msq_ref, msq_hbm))
    small = [pltpu.make_async_copy(src, dst, small_sem.at[k]) for k, (src, dst) in enumerate(pairs)]

    @pl.loop(0, blocks)
    def _(b):
        slot = lax.rem(b, SLOTS)

        @pl.when(b >= SLOTS)
        def _():
            out_copy(b - SLOTS).wait()

        cols = pl.ds(pl.multiple_of(b * block, LANES), block)
        factor = [jnp.broadcast_to(factor_ref.at[:, cols][:, TILE[k]] * common, (ROWS, LANES)) for k in range(block // LANES)]

        @pl.loop(0, rows // BLOCK)
        def _(i):
            at = pl.ds(pl.multiple_of(i * BLOCK, BLOCK), BLOCK)
            w, u, target = w_ref.at[at, cols], u_ref.at[at, cols], stage.at[slot, at]
            for row in ROW:
                for k in range(block // LANES):
                    new = w[row, TILE[k]].astype(jnp.float32) - u[row, TILE[k]] * factor[k]
                    target[row, TILE[k]] = new.astype(jnp.bfloat16)

        out_copy(b).start()

        @pl.when(b == 0)
        def _():
            for copy in small:
                copy.start()

    for copy in small:
        copy.wait()
    for b in range(max(blocks - SLOTS, 0), blocks):
        out_copy(b).wait()


def tile_count(width):
    total = width // LANES
    for d in (14, 7, 8, 4, 2, 1):
        if total % d == 0:
            return d


def block_width(columns):
    tiles = columns // LANES
    for d in (8, 7, 4, 2, 1):
        if tiles % d == 0:
            return d * LANES


def shards(step, gradient, weight, row_state, col_state, prev_msq):
    _, rows, columns = gradient.shape
    n = lax.axis_size("rows")
    experts = lax.axis_size("expert")
    width = columns // n
    f32, bf16 = jnp.float32, gradient.dtype
    vmem = pl.BlockSpec(memory_space=pltpu.VMEM)
    hbm = pl.BlockSpec(memory_space=pltpu.HBM)
    dma = pltpu.SemaphoreType.DMA
    u, w, factor, common, new_row, new_col, moved = pl.pallas_call(
        functools.partial(statistics_kernel, n, experts),
        out_shape=[
            pltpu.VMEM((rows, columns), f32),
            pltpu.VMEM((rows, columns), bf16),
            pltpu.VMEM((1, columns), f32),
            pltpu.VMEM((1, LANES), f32),
            pltpu.VMEM((1, rows), f32),
            pltpu.VMEM((1, width), f32),
            pltpu.VMEM((1, LANES), f32),
        ],
        in_specs=[pl.BlockSpec(memory_space=pltpu.SMEM)] * 2 + [hbm] * 4,
        out_specs=[vmem] * 7,
        scratch_shapes=[
            pltpu.VMEM((rows, LANES), f32),
            pltpu.VMEM((rows, LANES), f32),
            pltpu.VMEM((1, columns), f32),
            pltpu.VMEM((n, 1, width), f32),
            pltpu.VMEM((n - 1, 1, width), f32),
            pltpu.VMEM((1, width + 2 * LANES), f32),
            pltpu.VMEM((n - 1, 1, width + 2 * LANES), f32),
            pltpu.VMEM((1, LANES), f32),
            pltpu.VMEM((experts - 1, 1, LANES), f32),
            pltpu.VMEM((1, rows), f32),
            pltpu.VMEM((1, width), f32),
            dma((2,)), dma((DEPTH,)), dma, dma, dma, dma, dma, dma, dma((n - 1,)),
        ],
        compiler_params=pltpu.CompilerParams(
            collective_id=0, has_side_effects=True, vmem_limit_bytes=8 * 2**20
        ),
        name="statistics",
    )(
        step.reshape(1), prev_msq.reshape(1),
        *(
            pltpu.with_memory_space_constraint(x, pltpu.HBM)
            for x in (
                row_state, col_state,
                gradient.reshape(rows, columns), weight.reshape(rows, columns),
            )
        ),
    )
    block = block_width(columns)
    new_weight, new_row, new_col, msq = pl.pallas_call(
        functools.partial(update_kernel, block),
        out_shape=[
            jax.ShapeDtypeStruct((rows, columns), bf16),
            jax.ShapeDtypeStruct((1, rows), f32),
            jax.ShapeDtypeStruct((1, width), f32),
            jax.ShapeDtypeStruct((1, 1), f32),
        ],
        in_specs=[vmem] * 7,
        out_specs=[hbm] * 4,
        scratch_shapes=[pltpu.VMEM((SLOTS, rows, block), bf16), pltpu.VMEM((1, 1), f32), dma((SLOTS,)), dma((3,))],
        compiler_params=pltpu.CompilerParams(vmem_limit_bytes=8 * 2**20),
        name="update",
    )(u, w, factor, common, new_row, new_col, moved)
    return (new_weight.reshape(1, rows, columns), new_row, new_col, msq)


def solution(mesh):
    split = P("expert", "rows")
    whole = P("expert", "rows", None)
    return jax.shard_map(
        shards,
        mesh=mesh,
        in_specs=(P(), whole, whole, split, split, split),
        out_specs=(whole, split, split, split),
        check_vma=False,
    )
```

```python
import functools

import jax
import jax.numpy as jnp
from jax import lax
from jax.experimental import pallas as pl
from jax.experimental.pallas import tpu as pltpu
from jax.sharding import PartitionSpec as P

MESH = pl.DeviceIdType.MESH
RATE = 0.01
TINY = 1e-30
LANES = 128
ROWS = 16
BLOCK = 128
DEPTH = 4
EARLY = 2
SLOTS = 8
ROW = [slice(r, r + ROWS) for r in range(0, BLOCK, ROWS)]
TILE = [slice(k * LANES, (k + 1) * LANES) for k in range(16)]


def lane_sum(x):
    total = x[:, :LANES]
    for k in range(1, x.shape[1] // LANES):
        total = total + x[:, k * LANES : (k + 1) * LANES]
    return total


def statistics_kernel(
    n, experts, step_ref, prev_ref, row_hbm, col_hbm, g_hbm, w_hbm,
    u_out, w_out, factor_out, common_out, new_row_out, new_col_out, moved_out,
    acc, scale_ref, energy, part, parts_in, raws_in, message, messages_in, clip_out, clips_in,
    row_ref, col_ref, small_sem, g_sem, w_sem,
    clip_send, clip_recv, part_send, part_recv, raw_send, raw_recv, gather_send, gather_recv,
):
    me = lax.axis_index("rows")
    mine = lax.axis_index("expert")
    rows, columns = u_out.shape
    width = columns // n

    def column_slice(c):
        return pl.ds(pl.multiple_of(c * width, LANES), width)

    tiles = tile_count(width)

    def strip_slice(c, first):
        return pl.ds(pl.multiple_of(c * width + first * LANES, LANES), tiles * LANES)

    def partner(k):
        peer, bit = 0, 1
        while bit < n:
            peer = peer + bit * ((me // bit + k // bit) % 2)
            bit *= 2
        return peer

    def chunk_of(s):
        return partner(n - 1 - s)

    def g_copy(s):
        cols = column_slice(chunk_of(s))
        return pltpu.make_async_copy(g_hbm.at[:, cols], w_out.at[:, cols], g_sem.at[lax.rem(s, DEPTH)])

    def w_copy(s):
        cols = column_slice(s)
        return pltpu.make_async_copy(w_hbm.at[:, cols], w_out.at[:, cols], w_sem)

    def clip_copy(k):
        peer = lax.rem(mine + k, experts)
        return pltpu.make_async_remote_copy(
            src_ref=clip_out, dst_ref=clips_in.at[k - 1], send_sem=clip_send,
            recv_sem=clip_recv, device_id={"expert": peer}, device_id_type=MESH,
        )

    def part_copy(s):
        c = chunk_of(s)
        return pltpu.make_async_remote_copy(
            src_ref=part.at[s], dst_ref=parts_in.at[s], send_sem=part_send,
            recv_sem=part_recv, device_id={"rows": c}, device_id_type=MESH,
        )

    def raw_copy(s, k):
        return pltpu.make_async_remote_copy(
            src_ref=part.at[s], dst_ref=raws_in.at[n - 2 - s, k - 1], send_sem=raw_send,
            recv_sem=raw_recv, device_id={"rows": partner(k)}, device_id_type=MESH,
        )

    def gather_copy(k):
        peer = partner(k)
        return pltpu.make_async_remote_copy(
            src_ref=message, dst_ref=messages_in.at[k - 1], send_sem=gather_send,
            recv_sem=gather_recv.at[k - 1], device_id={"rows": peer}, device_id_type=MESH,
        )

    pairs = ((row_hbm, row_ref), (col_hbm, col_ref))
    small = [pltpu.make_async_copy(src, dst, small_sem.at[k]) for k, (src, dst) in enumerate(pairs)]
    for copy in small:
        copy.start()
    for s in range(DEPTH):
        g_copy(s).start()

    barrier = pltpu.get_barrier_semaphore()
    for k in range(1, n):
        pl.semaphore_signal(barrier, inc=1, device_id={"rows": lax.rem(me + k, n)}, device_id_type=MESH)
    for k in range(1, experts):
        pl.semaphore_signal(barrier, inc=1, device_id={"expert": lax.rem(mine + k, experts)}, device_id_type=MESH)

    clip_out[...] = jnp.full((1, LANES), prev_ref[0], jnp.float32)
    beta = 1.0 - jnp.exp(-0.8 * jnp.log(jnp.full((1, LANES), step_ref[0], jnp.int32).astype(jnp.float32)))

    def chunk(s):
        for first in range(0, width // LANES, tiles):
            strip = strip_slice(chunk_of(s), first)

            def body(i, carry):
                at = pl.ds(pl.multiple_of(i * BLOCK, BLOCK), BLOCK)
                source, target = w_out.at[at, strip], u_out.at[at, strip]
                carry = list(carry)
                for row in ROW:
                    for k in range(tiles):
                        x = source[row, TILE[k]].astype(jnp.float32)
                        target[row, TILE[k]] = x
                        squares = x * x
                        carry[k] = carry[k] + (squares[: ROWS // 2] + squares[ROWS // 2 :])
                return tuple(carry)

            zeros = (jnp.zeros((ROWS // 2, LANES), jnp.float32),) * tiles
            col = lax.fori_loop(0, rows // BLOCK, body, zeros)
            for k in range(tiles):
                part[s, :, (first + k) * LANES : (first + k + 1) * LANES] = jnp.sum(col[k], axis=0, keepdims=True)

    def scaled(s):
        for first in range(0, width // LANES, tiles):
            strip = strip_slice(s, first)

            def body(i, carry):
                at = pl.ds(pl.multiple_of(i * BLOCK, BLOCK), BLOCK)
                target, scales = u_out.at[at, strip], scale_ref.at[at]
                carry = list(carry)
                for row in ROW:
                    scale = scales[row, :]
                    for k in range(tiles):
                        u = target[row, TILE[k]] * scale
                        target[row, TILE[k]] = u
                        squares = u * u
                        carry[k] = carry[k] + (squares[: ROWS // 2] + squares[ROWS // 2 :])
                return tuple(carry)

            zeros = (jnp.zeros((ROWS // 2, LANES), jnp.float32),) * tiles
            col = lax.fori_loop(0, rows // BLOCK, body, zeros)
            for k in range(tiles):
                energy.at[:, strip][:, TILE[k]] = jnp.sum(col[k], axis=0, keepdims=True)

    ready = jnp.where(me == 0, n - 3, jnp.where(me >= n // 2, 1, n // 2))

    @pl.loop(0, n - 1)
    def _(s):
        g_copy(s).wait()

        @pl.when(s + DEPTH < n)
        def _():
            g_copy(s + DEPTH).start()

        @pl.when(s + DEPTH >= n)
        def _():
            w_copy(chunk_of(s + DEPTH - n)).start()

        chunk(s)

        @pl.when(s + 1 == ready)
        def _():
            pl.semaphore_wait(barrier, n - 1 + experts - 1)
            for k in range(1, experts):
                clip_copy(k).start()

            @pl.loop(0, s)
            def _(t):
                part_copy(t).start()

        @pl.when(jnp.logical_and(s + 1 >= ready, s < n - 3))
        def _():
            part_copy(s).start()

        @pl.when(s >= n - 3)
        def _():
            for k in reversed(range(1, n)):
                raw_copy(s, k).start()

    g_copy(n - 1).wait()
    for s in range(DEPTH - 1, n - 1):
        w_copy(chunk_of(s)).start()
    chunk(n - 1)
    w_copy(chunk_of(n - 1)).start()

    for copy in small:
        copy.wait()
    beta_rows = jnp.concatenate([beta] * (rows // LANES), axis=1)
    squares = part[0]
    for s in range(1, n):
        squares = squares + part[s]
    beta_cols = jnp.concatenate([beta] * (width // LANES), axis=1)
    weight = (1.0 - beta_cols) * (1.0 / (rows * n))
    share = lane_sum(row_ref[...]) * beta
    share = share + (1.0 - beta) * (lane_sum(squares) * (1.0 / columns) + TINY * (rows / LANES))
    share = jnp.broadcast_to(jnp.sum(share, axis=1, keepdims=True), (1, LANES))

    def whole_copy(ref, send, recv):
        return pltpu.make_async_remote_copy(
            src_ref=ref, dst_ref=ref, send_sem=send, recv_sem=recv,
            device_id={"rows": partner(1)}, device_id_type=MESH,
        )

    def respond():
        clips = clip_out[...]
        whole_copy(clips_in, clip_send, clip_recv).wait()
        for k in range(1, experts):
            clips = clips + clips_in[k - 1]
        whole_copy(parts_in, part_send, part_recv).wait_recv()
        total = part[n - 1]
        for s in range(n - 3):
            total = total + parts_in[s]
        message[:, :width] = beta_cols * col_ref[...] + (1.0 - beta_cols) * TINY + weight * total
        message[:, width : width + LANES] = share
        message[:, width + LANES :] = clips
        for k in reversed(range(1, n)):
            gather_copy(k).start()

    def row_sums(i):
        at = pl.ds(pl.multiple_of(i * ROWS, ROWS), ROWS)
        source = u_out.at[at]
        sums = [None] * 4
        for k in range(columns // LANES):
            x = source[:, k * LANES : (k + 1) * LANES]
            sums[k % 4] = x * x if k < 4 else sums[k % 4] + x * x
        acc[at, :] = (sums[0] + sums[1]) + (sums[2] + sums[3])

    middle = rows // ROWS // 2

    @pl.loop(0, middle)
    def _(i):
        row_sums(i)

    @pl.when(me != 0)
    def _():
        respond()

    @pl.loop(middle, rows // ROWS)
    def _(i):
        row_sums(i)

    sums = jnp.sum(jnp.transpose(acc[...]), axis=0, keepdims=True)
    new_row = beta_rows * row_ref[...] + (1.0 - beta_rows) * (sums * (1.0 / columns) + TINY)
    new_row_out[...] = new_row
    scale_ref[...] = jnp.transpose(jnp.broadcast_to(lax.rsqrt(new_row), (LANES, rows)))
    early = jnp.where(me == 0, n * EARLY // 8, 0)

    @pl.loop(0, early)
    def _(s):
        scaled(s)

    @pl.when(me == 0)
    def _():
        respond()

    @pl.loop(early, n)
    def _(s):
        scaled(s)

    pltpu.make_async_copy(w_hbm, w_out, w_sem).wait()

    whole_copy(parts_in, part_send, part_recv).wait_send()
    whole_copy(raws_in, raw_send, raw_recv).wait()
    share, clips, moved = 0.0, 0.0, 0.0
    for k in range(n):
        cols = column_slice(partner(k))
        if k > 0:
            gather_copy(k).wait_recv()
        got = message[...] if k == 0 else messages_in[k - 1]
        raw = 0.0
        for x in range(1, 3):
            raw = raw + (part[n - 1 - x] if k == x else raws_in[x - 1, (k ^ x) - 1])
        column = got[:, :width] + weight * raw
        if k == 0:
            new_col_out[...] = column
        inverse = lax.rsqrt(column)
        factor_out[:, cols] = inverse
        share = share + got[:, width : width + LANES]
        clips = clips + got[:, width + LANES :]
        moved = moved + lane_sum(energy[:, cols] * (inverse * inverse))
    whole_copy(messages_in, gather_send, gather_recv.at[0]).wait_send()
    common_out[...] = RATE * jnp.sqrt(share * (1.0 / (rows * n))) * lax.rsqrt(clips * (1.0 / (n * experts)))
    moved_out[...] = moved


def update_kernel(
    block, u_ref, w_ref, factor_ref, common_ref, row_ref, col_ref, moved_ref,
    new_w_hbm, new_row_hbm, new_col_hbm, msq_hbm, stage, msq_ref, sem, small_sem,
):
    rows, columns = u_ref.shape
    blocks = columns // block
    common = common_ref[...]
    msq = moved_ref[...] * (common * common) * (1.0 / (RATE * RATE * rows * columns))
    msq_ref[...] = jnp.sum(msq, axis=1, keepdims=True)

    def out_copy(b):
        slot = lax.rem(b, SLOTS)
        cols = pl.ds(pl.multiple_of(b * block, LANES), block)
        return pltpu.make_async_copy(stage.at[slot], new_w_hbm.at[:, cols], sem.at[slot])

    pairs = ((row_ref, new_row_hbm), (col_ref, new_col_hbm), (msq_ref, msq_hbm))
    small = [pltpu.make_async_copy(src, dst, small_sem.at[k]) for k, (src, dst) in enumerate(pairs)]

    @pl.loop(0, blocks)
    def _(b):
        slot = lax.rem(b, SLOTS)

        @pl.when(b >= SLOTS)
        def _():
            out_copy(b - SLOTS).wait()

        cols = pl.ds(pl.multiple_of(b * block, LANES), block)
        factor = [jnp.broadcast_to(factor_ref.at[:, cols][:, TILE[k]] * common, (ROWS, LANES)) for k in range(block // LANES)]

        w, u = w_ref.at[:, cols], u_ref.at[:, cols]
        for r in range(0, rows, ROWS):
            row = slice(r, r + ROWS)
            for k in range(block // LANES):
                new = w[row, TILE[k]].astype(jnp.float32) - u[row, TILE[k]] * factor[k]
                stage[slot, row, TILE[k]] = new.astype(jnp.bfloat16)

        out_copy(b).start()

        @pl.when(b == 0)
        def _():
            for copy in small:
                copy.start()

    for copy in small:
        copy.wait()
    for b in range(max(blocks - SLOTS, 0), blocks):
        out_copy(b).wait()


def tile_count(width):
    total = width // LANES
    for d in (14, 7, 8, 4, 2, 1):
        if total % d == 0:
            return d


def block_width(columns):
    tiles = columns // LANES
    for d in (4, 2, 1):
        if tiles % d == 0:
            return d * LANES


def shards(step, gradient, weight, row_state, col_state, prev_msq):
    _, rows, columns = gradient.shape
    n = lax.axis_size("rows")
    experts = lax.axis_size("expert")
    width = columns // n
    f32, bf16 = jnp.float32, gradient.dtype
    vmem = pl.BlockSpec(memory_space=pltpu.VMEM)
    hbm = pl.BlockSpec(memory_space=pltpu.HBM)
    dma = pltpu.SemaphoreType.DMA
    u, w, factor, common, new_row, new_col, moved = pl.pallas_call(
        functools.partial(statistics_kernel, n, experts),
        out_shape=[
            pltpu.VMEM((rows, columns), f32),
            pltpu.VMEM((rows, columns), bf16),
            pltpu.VMEM((1, columns), f32),
            pltpu.VMEM((1, LANES), f32),
            pltpu.VMEM((1, rows), f32),
            pltpu.VMEM((1, width), f32),
            pltpu.VMEM((1, LANES), f32),
        ],
        in_specs=[pl.BlockSpec(memory_space=pltpu.SMEM)] * 2 + [hbm] * 4,
        out_specs=[vmem] * 7,
        scratch_shapes=[
            pltpu.VMEM((rows, LANES), f32),
            pltpu.VMEM((rows, LANES), f32),
            pltpu.VMEM((1, columns), f32),
            pltpu.VMEM((n, 1, width), f32),
            pltpu.VMEM((n - 3, 1, width), f32),
            pltpu.VMEM((2, n - 1, 1, width), f32),
            pltpu.VMEM((1, width + 2 * LANES), f32),
            pltpu.VMEM((n - 1, 1, width + 2 * LANES), f32),
            pltpu.VMEM((1, LANES), f32),
            pltpu.VMEM((experts - 1, 1, LANES), f32),
            pltpu.VMEM((1, rows), f32),
            pltpu.VMEM((1, width), f32),
            dma((2,)), dma((DEPTH,)), dma, dma, dma, dma, dma, dma, dma, dma, dma((n - 1,)),
        ],
        compiler_params=pltpu.CompilerParams(
            collective_id=0, has_side_effects=True, vmem_limit_bytes=8 * 2**20
        ),
        name="statistics",
    )(
        step.reshape(1), prev_msq.reshape(1),
        *(
            pltpu.with_memory_space_constraint(x, pltpu.HBM)
            for x in (
                row_state, col_state,
                gradient.reshape(rows, columns), weight.reshape(rows, columns),
            )
        ),
    )
    block = block_width(columns)
    new_weight, new_row, new_col, msq = pl.pallas_call(
        functools.partial(update_kernel, block),
        out_shape=[
            jax.ShapeDtypeStruct((rows, columns), bf16),
            jax.ShapeDtypeStruct((1, rows), f32),
            jax.ShapeDtypeStruct((1, width), f32),
            jax.ShapeDtypeStruct((1, 1), f32),
        ],
        in_specs=[vmem] * 7,
        out_specs=[hbm] * 4,
        scratch_shapes=[pltpu.VMEM((SLOTS, rows, block), bf16), pltpu.VMEM((1, 1), f32), dma((SLOTS,)), dma((3,))],
        compiler_params=pltpu.CompilerParams(vmem_limit_bytes=8 * 2**20),
        name="update",
    )(u, w, factor, common, new_row, new_col, moved)
    return (new_weight.reshape(1, rows, columns), new_row, new_col, msq)


def solution(mesh):
    split = P("expert", "rows")
    whole = P("expert", "rows", None)
    return jax.shard_map(
        shards,
        mesh=mesh,
        in_specs=(P(), whole, whole, split, split, split),
        out_specs=(whole, split, split, split),
        check_vma=False,
    )
```
